256 devices in a mesh: section: 4 (over y_hi, core), replica: 64 (over x, z, y_lo).
Axes of the slice: x: 4, y: 4 (y_hi: 2, y_lo: 2; y = y_hi * 2 + y_lo), z: 8, core: 2. Of those that a mesh axis runs over, the one named last changes fastest.
Arguments:
- tokens: bfloat16 [64, 128, 2048], P('replica', 'section'), may hold values from -6 to 6
- gate_weight: bfloat16 [4, 64, 2048, 384], P('section', 'replica'), may hold values from -0.125 to 0.125
- up_weight: bfloat16 [4, 64, 2048, 384], P('section', 'replica'), may hold values from -0.125 to 0.125
- slow_down: float32 [4, 64, 384, 2048], P('section', 'replica'), may hold values from -0.3125 to 0.3125
- prev_outer: bfloat16 [4, 64, 384, 2048], P('section', 'replica'), may hold values from -0.29882812 to 0.29882812
- route: int32 [3, 1, 64], replicated, may hold values from 0 to 63, each once within a row
- partner: int32 [64], replicated, may hold values from 0 to 63, as said below
Outputs:
- new_slow: float32 [4, 64, 384, 2048], P('section', 'replica')
- new_outer: bfloat16 [4, 64, 384, 2048], P('section', 'replica')
The draws below stay inside these ranges and needn't reach their ends.
Inputs may be any that keep to these rules, and one draw needn't show every extreme that they name: route[s, m] is a permutation of the replicas: replica r at section s hands micro-batch m to replica route[s, m, r] at section s + 1. partner pairs the replicas: partner[partner[r]] = r and partner[r] != r.
All inputs are finite; a program needn't handle non-finite values.
Results may differ from the reference program's by a relative error of at most 0.017.
Values may be sent and summed in bfloat16 or wider, within the bound.
A program may use at most 128 MiB of HBM per device.

```python
import jax
import jax.numpy as jnp
from jax import lax

D = 2048
HID = 384
MT = 128
MB = 1
N_SECTION = 4
N_REPLICA = 64


def draw_partner(key, part):
    shuffled = jax.random.permutation(jax.random.fold_in(key, 7), N_REPLICA).astype(jnp.int32)
    paired = shuffled.reshape(-1, 2)
    result = jnp.zeros((N_REPLICA,), jnp.int32)
    result = result.at[paired[:, 0]].set(paired[:, 1])
    result = result.at[paired[:, 1]].set(paired[:, 0])
    return result


def shard_levels(stream_key, dims, pieces, low, top_value):
    loudness, own = 1.0, jax.random.fold_in(stream_key, 6)
    for dim, blocks in pieces:
        draws = jnp.exp(jax.random.uniform(jax.random.fold_in(own, dim), (blocks,), jnp.float32, low / len(pieces), top_value / len(pieces)))
        loudness = loudness * jnp.repeat(draws, dims[dim] // blocks).reshape([-1 if axis == dim else 1 for axis in range(len(dims))])
    return loudness


def gaussian(rng, extent, width, reach, split=(), kind=jnp.bfloat16):
    loudness = shard_levels(rng, extent, split, -0.22, 0.18) if split else 1.0
    array = jax.random.normal(rng, extent, jnp.float32) * width * loudness
    return jnp.minimum(jnp.maximum(array, -reach), reach).astype(kind)


def setup_inputs(seed: int = 0) -> dict:
    arg_keys = jax.random.split(jax.random.key(seed), 8)
    return {
        "tokens": gaussian(arg_keys[0], (N_REPLICA, MB * MT, D), 1.0, 6.0, ((0, 64), (1, 4))),
        "gate_weight": gaussian(arg_keys[1], (N_SECTION, N_REPLICA, D, HID), D ** -0.5, 0.125, ((0, 4), (1, 64))),
        "up_weight": gaussian(arg_keys[2], (N_SECTION, N_REPLICA, D, HID), D ** -0.5, 0.125, ((0, 4), (1, 64))),
        "slow_down": gaussian(arg_keys[3], (N_SECTION, N_REPLICA, HID, D), HID ** -0.5, 0.3125, ((0, 4), (1, 64)), jnp.float32),
        "prev_outer": gaussian(arg_keys[4], (N_SECTION, N_REPLICA, HID, D), 0.05, 0.29882812, ((0, 4), (1, 64))),
        "route": jax.vmap(lambda own: jax.random.permutation(own, N_REPLICA))(jax.random.split(arg_keys[5], (N_SECTION - 1) * MB)).reshape((N_SECTION - 1, MB, N_REPLICA)).astype(jnp.int32),
        "partner": draw_partner(jax.random.fold_in(arg_keys[7], 71), 0),
    }


EPSILON = 1e-05
OUTER_RATE = 0.7
MOMENTUM = 0.9

def section_forward(inputs, gate_w, up_w, down_w):
    widened = inputs.astype(jnp.float32)
    inv_rms = lax.rsqrt(lax.optimization_barrier(jnp.mean(widened * widened, axis=-1, keepdims=True)) + EPSILON)
    normed = (widened * inv_rms).astype(jnp.bfloat16)
    gate_act = jnp.dot(normed, gate_w, preferred_element_type=jnp.float32)
    up_act = jnp.dot(normed, up_w, preferred_element_type=jnp.float32)
    hidden = (jax.nn.silu(gate_act) * up_act).astype(jnp.bfloat16)
    output = (widened + jnp.dot(hidden, down_w, preferred_element_type=jnp.float32)).astype(jnp.bfloat16)
    return (output, gate_act, up_act, hidden)

def section_backward(inputs, gate_act, up_act, hidden, upstream, gate_w, up_w, down_w):
    contract_rows = (((0,), (0,)), ((), ()))
    contract_cols = (((1,), (1,)), ((), ()))
    grad_part = lax.dot_general(hidden, upstream, contract_rows, preferred_element_type=jnp.float32)
    hidden_grad = lax.dot_general(upstream, down_w, contract_cols, preferred_element_type=jnp.float32)
    sigmoid_gate = jax.nn.sigmoid(gate_act)
    gate_grad = (hidden_grad * up_act * sigmoid_gate * (1.0 + gate_act * (1.0 - sigmoid_gate))).astype(jnp.bfloat16)
    up_grad = (hidden_grad * gate_act * sigmoid_gate).astype(jnp.bfloat16)
    normed_grad = lax.dot_general(gate_grad, gate_w, contract_cols, preferred_element_type=jnp.float32)
    normed_grad = normed_grad + lax.dot_general(up_grad, up_w, contract_cols, preferred_element_type=jnp.float32)
    widened = inputs.astype(jnp.float32)
    inv_rms = lax.rsqrt(lax.optimization_barrier(jnp.mean(widened * widened, axis=-1, keepdims=True)) + EPSILON)
    input_grad = upstream.astype(jnp.float32) + inv_rms * normed_grad
    input_grad = input_grad - widened * inv_rms ** 3 * lax.optimization_barrier(jnp.mean(normed_grad * widened, axis=-1, keepdims=True))
    return (grad_part, input_grad.astype(jnp.bfloat16))

def reference(tokens, gate_weight, up_weight, slow_down, prev_outer, route, partner):
    current = tokens.reshape(N_REPLICA, MB, MT, D)
    saved = []
    produced = current
    for section_index in range(N_SECTION):
        down_fast = slow_down[section_index].astype(jnp.bfloat16)

        def run_forward(packed):
            rows, gate_w, up_w, down_w = packed
            output, gate_act, up_act, hidden = section_forward(rows.reshape(MB * MT, D), gate_w, up_w, down_w)
            return (output.reshape(MB, MT, D), gate_act, up_act, hidden)
        results = lax.map(run_forward, (current, gate_weight[section_index], up_weight[section_index], down_fast))
        saved.append((current, results[1], results[2], results[3], down_fast))
        produced = results[0]
        if section_index < N_SECTION - 1:
            routed = []
            for micro_index in range(MB):
                empty = jnp.zeros_like(produced[:, micro_index])
                routed.append(empty.at[route[section_index, micro_index]].set(produced[:, micro_index]))
            current = jnp.stack(routed, axis=1)
    upstream = (produced.astype(jnp.float32) / float(MB * MT)).astype(jnp.bfloat16)
    weight_grads = [None] * N_SECTION
    for section_index in range(N_SECTION - 1, -1, -1):
        inputs, gate_act, up_act, hidden, down_fast = saved[section_index]

        def run_backward(packed):
            rows, gate_a, up_a, hidden_a, upstream_a, gate_w, up_w, down_w = packed
            grad_part, input_grad = section_backward(rows.reshape(MB * MT, D), gate_a, up_a, hidden_a, upstream_a.reshape(MB * MT, D), gate_w, up_w, down_w)
            return (grad_part, input_grad.reshape(MB, MT, D))
        grad_part, input_grad = lax.map(run_backward, (inputs, gate_act, up_act, hidden, upstream, gate_weight[section_index], up_weight[section_index], down_fast))
        weight_grads[section_index] = grad_part
        if section_index > 0:
            upstream = jnp.stack([input_grad[route[section_index - 1, micro_index], micro_index] for micro_index in range(MB)], axis=1)
    weight_grad = jnp.stack(weight_grads)
    average_slow = 0.5 * (slow_down + slow_down[:, partner])
    average_prev = 0.5 * (prev_outer.astype(jnp.float32) + prev_outer[:, partner].astype(jnp.float32))
    velocity = MOMENTUM * average_prev + weight_grad
    new_slow = average_slow - OUTER_RATE * (weight_grad + MOMENTUM * velocity)
    return (new_slow, velocity.astype(jnp.bfloat16))
```

```python
import functools

import jax
import jax.numpy as jnp
from jax import lax
from jax.experimental import pallas as pl
from jax.experimental.pallas import tpu as pltpu
from jax.sharding import PartitionSpec as P

EPSILON = 1e-05
OUTER_RATE = 0.7
MOMENTUM = 0.9

MESH = pl.DeviceIdType.MESH
F32 = jnp.float32
BF16 = jnp.bfloat16

NN = (((1,), (0,)), ((), ()))
NT = (((1,), (1,)), ((), ()))
TN = (((0,), (0,)), ((), ()))


def dot(a, b, dims):
    return lax.dot_general(a, b, dims, preferred_element_type=F32)


def kernel(
    sections,
    replicas,
    stride,
    source_ref,
    tokens_ref,
    gate_ref,
    up_ref,
    slow_ref,
    prev_ref,
    new_slow_ref,
    new_outer_ref,
    gate_w,
    up_w,
    slow_w,
    pair_w,
    act,
    out,
    upstream,
    grad,
    spread_in_0,
    spread_in_1,
    spread_out_0,
    spread_out_1,
    gossip_in_0,
    gossip_in_1,
    gossip_out_0,
    gossip_out_1,
    mate,
    velocity,
    inv_rms,
    gate_act,
    up_act,
    hidden,
    load_sem,
    store_sem,
    token_send,
    token_recv,
    first_send,
    first_recv,
    second_send,
    second_recv,
    gossip_send,
    gossip_recv,
):
    spread_in = (spread_in_0, spread_in_1)
    spread_out = (spread_out_0, spread_out_1)
    gossip_in = (gossip_in_0, gossip_in_1)
    gossip_out = (gossip_out_0, gossip_out_1)
    section = lax.axis_index("section")
    replica = lax.axis_index("replica")
    rows, features = act.shape
    units = pair_w.shape[1]
    across = features // spread_in_0.shape[2]
    down = replicas // across

    def load(ref, target, index):
        return pltpu.make_async_copy(ref, target, load_sem.at[index])

    loads = (
        load(slow_ref, slow_w, 0),
        load(prev_ref, pair_w.at[1], 1),
        load(gate_ref, gate_w, 2),
        load(up_ref, up_w, 3),
    )
    for copy in loads:
        copy.start()

    barrier = pltpu.get_barrier_semaphore()

    def greet(target):
        def one(step, carry):
            pl.semaphore_signal(
                barrier,
                inc=1,
                device_id=(target, lax.rem(replica + step, replicas)),
                device_id_type=MESH,
            )
            return carry

        lax.fori_loop(0, replicas, one, 0)

    for target in range(sections):

        @pl.when(section != target)
        def _():
            greet(target)

    def greet_own(step, carry):
        pl.semaphore_signal(
            barrier,
            inc=1,
            device_id=(section, lax.rem(replica + step, replicas)),
            device_id_type=MESH,
        )
        return carry

    lax.fori_loop(1, replicas, greet_own, 0)
    pl.semaphore_wait(barrier, sections * replicas - 1)

    band = rows // sections

    def token_copy(origin):
        return pltpu.make_async_remote_copy(
            src_ref=tokens_ref,
            dst_ref=act.at[pl.ds(pl.multiple_of(origin * band, band), band)],
            send_sem=token_send,
            recv_sem=token_recv,
            device_id=(0, replica),
            device_id_type=MESH,
        )

    @pl.when(section != 0)
    def _():
        token_copy(section).start()

    @pl.when(section == 0)
    def _():
        pltpu.make_async_copy(tokens_ref, act.at[pl.ds(0, band)], token_recv).start()

    def area(ref, index):
        tall, wide = ref.shape[0] // down, ref.shape[1] // across
        top = pl.multiple_of(lax.div(index, across) * tall, tall)
        left = pl.multiple_of(lax.rem(index, across) * wide, wide)
        return ref.at[pl.ds(top, tall), pl.ds(left, wide)]

    def other(step):
        return lax.rem(replica + step * stride, replicas)

    def spread(ref, target, way):
        def one(step, carry):
            peer = other(step)
            pltpu.make_async_remote_copy(
                src_ref=area(ref, peer),
                dst_ref=spread_in[way].at[replica],
                send_sem=first_send.at[way],
                recv_sem=first_recv.at[way],
                device_id=(target, peer),
                device_id_type=MESH,
            ).start()
            return carry

        lax.fori_loop(0, replicas, one, 0)

    def spread_done(ref, way):
        pltpu.make_async_copy(ref, ref, first_send.at[way]).wait()

    def gather(ref, table, way):
        pltpu.make_async_copy(
            spread_in[way], spread_in[way], first_recv.at[way]
        ).wait()

        def pick(step, carry):
            spread_out[way][step] = spread_in[way][source_ref[table, step]]
            return carry

        lax.fori_loop(0, replicas, pick, 0, unroll=8)
        pltpu.make_async_copy(
            spread_out[way].at[replica], area(ref, replica), second_recv.at[way]
        ).start()

        def one(step, carry):
            peer = other(step)
            pltpu.make_async_remote_copy(
                src_ref=spread_out[way].at[peer],
                dst_ref=area(ref, replica),
                send_sem=second_send.at[way],
                recv_sem=second_recv.at[way],
                device_id=(section, peer),
                device_id_type=MESH,
            ).start()
            return carry

        lax.fori_loop(1, replicas, one, 0)
        pltpu.make_async_copy(ref, ref, second_recv.at[way]).wait()

    def gather_done(way):
        part = spread_out[way].at[pl.ds(0, replicas - 1)]
        pltpu.make_async_copy(part, part, second_send.at[way]).wait()

    def gossip_first(part):
        pltpu.make_async_copy(
            area(pair_w.at[part], replica),
            gossip_in[part].at[replica],
            gossip_recv.at[part],
        ).start()

        def one(step, carry):
            peer = other(step)
            pltpu.make_async_remote_copy(
                src_ref=area(pair_w.at[part], peer),
                dst_ref=gossip_in[part].at[replica],
                send_sem=gossip_send.at[part],
                recv_sem=gossip_recv.at[part],
                device_id=(section, peer),
                device_id_type=MESH,
            ).start()
            return carry

        lax.fori_loop(1, replicas, one, 0)

    def gossip_second(part):
        pltpu.make_async_copy(
            gossip_in[part], gossip_in[part], gossip_recv.at[part]
        ).wait()

        def pick(step, carry):
            gossip_out[part][step] = gossip_in[part][source_ref[2 * sections - 2, step]]
            return carry

        lax.fori_loop(0, replicas, pick, 0, unroll=4)
        pltpu.make_async_copy(
            gossip_out[part].at[replica],
            area(mate.at[part], replica),
            gossip_recv.at[2 + part],
        ).start()

        def one(step, carry):
            peer = other(step)
            pltpu.make_async_remote_copy(
                src_ref=gossip_out[part].at[peer],
                dst_ref=area(mate.at[part], replica),
                send_sem=gossip_send.at[2 + part],
                recv_sem=gossip_recv.at[2 + part],
                device_id=(section, peer),
                device_id_type=MESH,
            ).start()
            return carry

        lax.fori_loop(1, replicas, one, 0)

    def gossip_done(part):
        for stage in range(2):
            piece = gossip_out[part].at[pl.ds(0, replicas - 1)]
            pltpu.make_async_copy(piece, piece, gossip_send.at[2 * stage + part]).wait()

    loads[0].wait()
    pair_w[0] = slow_w[...].astype(BF16)
    loads[1].wait()

    @pl.when(section >= sections // 2)
    def _():
        gossip_first(0)

    loads[2].wait()
    loads[3].wait()

    @pl.when(section == 0)
    def _():
        pltpu.make_async_copy(act, act, token_recv).wait()

    @pl.when(section > 0)
    def _():
        gather(act, section - 1, 0)

    wide = act[...].astype(F32)
    scale = lax.rsqrt(jnp.mean(wide * wide, axis=-1, keepdims=True) + EPSILON)
    inv_rms[...] = scale
    normed = (wide * scale).astype(BF16)
    gate = dot(normed, gate_w[...], NN)
    up = dot(normed, up_w[...], NN)
    gate_act[...] = gate
    up_act[...] = up
    hid = (jax.nn.silu(gate) * up).astype(BF16)
    hidden[...] = hid
    result = (act[...].astype(F32) + dot(hid, pair_w[0], NN)).astype(BF16)
    out[...] = result

    @pl.when(section < sections - 1)
    def _():
        spread(out, section + 1, 0)

    @pl.when(section == sections - 1)
    def _():
        upstream[...] = (out[...].astype(F32) / float(rows)).astype(BF16)

    @pl.when(section < sections // 2)
    def _():
        gossip_first(0)
        gossip_first(1)

    @pl.when(section < sections - 1)
    def _():
        gather(upstream, sections - 1 + section, 1)

    above = upstream[...]
    hidden_grad = dot(above, pair_w[0], NT)
    gate = gate_act[...]
    sig = jax.nn.sigmoid(gate)
    gate_grad = (hidden_grad * up_act[...] * sig * (1.0 + gate * (1.0 - sig))).astype(BF16)
    up_grad = (hidden_grad * gate * sig).astype(BF16)

    @pl.when(section > 0)
    def _():
        normed_grad = dot(gate_grad, gate_w[...], NT) + dot(up_grad, up_w[...], NT)
        scale = inv_rms[...]
        wide = act[...].astype(F32)
        mean = jnp.mean(normed_grad * wide, axis=-1, keepdims=True)
        grad[...] = (
            upstream[...].astype(F32) + scale * normed_grad - wide * scale**3 * mean
        ).astype(BF16)
        spread(grad, section - 1, 1)

    @pl.when(section >= sections // 2)
    def _():
        gossip_first(1)

    weight_grad = dot(hidden[...], upstream[...], TN)
    old = pair_w[1].astype(F32)
    speed = (0.5 * MOMENTUM) * old + weight_grad
    velocity[...] = speed
    slow_w[...] = 0.5 * slow_w[...] - OUTER_RATE * (weight_grad + MOMENTUM * speed)

    gossip_second(0)
    gossip_second(1)

    @pl.when(section != 0)
    def _():
        pltpu.make_async_copy(tokens_ref, tokens_ref, token_send).wait()
        gather_done(0)
        spread_done(grad, 1)

    @pl.when(section < sections - 1)
    def _():
        spread_done(out, 0)
        gather_done(1)

    pltpu.make_async_copy(mate.at[0], mate.at[0], gossip_recv.at[2]).wait()
    pltpu.make_async_copy(mate.at[1], mate.at[1], gossip_recv.at[3]).wait()
    for part in range(2):
        gossip_done(part)
    theirs = (0.5 * MOMENTUM) * mate[1].astype(F32)
    slow_w[...] = slow_w[...] + (
        0.5 * mate[0].astype(F32) - (OUTER_RATE * MOMENTUM) * theirs
    )
    gossip = (velocity[...] + theirs).astype(BF16)
    pair_w[0] = gossip
    stores = (
        pltpu.make_async_copy(slow_w, new_slow_ref, store_sem.at[0]),
        pltpu.make_async_copy(pair_w.at[0], new_outer_ref, store_sem.at[1]),
    )
    for copy in stores:
        copy.start()
    for copy in stores:
        copy.wait()


def local(sections, replicas, tokens, gate_weight, up_weight, slow_down, prev_outer, route, partner):
    rows = tokens.shape[1] * sections
    features = tokens.shape[2]
    units = gate_weight.shape[3]
    order = jnp.arange(replicas, dtype=jnp.int32)
    targets = route[:, 0]
    origins = jnp.sum(
        jnp.where(targets[:, :, None] == order, order[:, None], 0), axis=1, dtype=jnp.int32
    )
    sources = jnp.concatenate([origins, targets, partner[None]], axis=0)
    across = min(16, replicas)
    down = replicas // across
    piece = (rows // down, features // across)
    share = (units // down, features // across)
    stride = 37 if replicas == 64 else 1
    anywhere = pl.BlockSpec(memory_space=pl.ANY)
    dma = pltpu.SemaphoreType.DMA
    new_slow, new_outer = pl.pallas_call(
        functools.partial(kernel, sections, replicas, stride),
        out_shape=(
            jax.ShapeDtypeStruct((units, features), F32),
            jax.ShapeDtypeStruct((units, features), BF16),
        ),
        in_specs=[pl.BlockSpec(memory_space=pltpu.SMEM)] + [anywhere] * 5,
        out_specs=(anywhere, anywhere),
        scratch_shapes=[
            pltpu.VMEM((features, units), BF16),
            pltpu.VMEM((features, units), BF16),
            pltpu.VMEM((units, features), F32),
            pltpu.VMEM((2, units, features), BF16),
            pltpu.VMEM((rows, features), BF16),
            pltpu.VMEM((rows, features), BF16),
            pltpu.VMEM((rows, features), BF16),
            pltpu.VMEM((rows, features), BF16),
            pltpu.VMEM((replicas, *piece), BF16),
            pltpu.VMEM((replicas, *piece), BF16),
            pltpu.VMEM((replicas, *piece), BF16),
            pltpu.VMEM((replicas, *piece), BF16),
            pltpu.VMEM((replicas, *share), BF16),
            pltpu.VMEM((replicas, *share), BF16),
            pltpu.VMEM((replicas, *share), BF16),
            pltpu.VMEM((replicas, *share), BF16),
            pltpu.VMEM((2, units, features), BF16),
            pltpu.VMEM((units, features), F32),
            pltpu.VMEM((rows, 1), F32),
            pltpu.VMEM((rows, units), F32),
            pltpu.VMEM((rows, units), F32),
            pltpu.VMEM((rows, units), BF16),
            dma((4,)),
            dma((2,)),
            dma,
            dma,
            dma((2,)),
            dma((2,)),
            dma((2,)),
            dma((2,)),
            dma((4,)),
            dma((4,)),
        ],
        compiler_params=pltpu.CompilerParams(
            collective_id=0, has_side_effects=True, vmem_limit_bytes=60 * 2**20
        ),
        name="relay",
    )(sources, tokens[0], gate_weight[0, 0], up_weight[0, 0], slow_down[0, 0], prev_outer[0, 0])
    return (new_slow[None, None], new_outer[None, None])


def solution(mesh):
    sections, replicas = mesh.shape["section"], mesh.shape["replica"]
    own = P("section", "replica", None, None)
    return jax.shard_map(
        functools.partial(local, sections, replicas),
        mesh=mesh,
        in_specs=(P("replica", "section", None), own, own, own, own, P(), P()),
        out_specs=(own, own),
        check_vma=False,
    )
```

```python
import functools

import jax
import jax.numpy as jnp
from jax import lax
from jax.experimental import pallas as pl
from jax.experimental.pallas import tpu as pltpu
from jax.sharding import PartitionSpec as P

EPSILON = 1e-05
OUTER_RATE = 0.7
MOMENTUM = 0.9

MESH = pl.DeviceIdType.MESH
F32 = jnp.float32
BF16 = jnp.bfloat16

NN = (((1,), (0,)), ((), ()))
NT = (((1,), (1,)), ((), ()))
TN = (((0,), (0,)), ((), ()))


def dot(a, b, dims):
    return lax.dot_general(a, b, dims, preferred_element_type=F32)


def kernel(
    sections,
    replicas,
    stride,
    torus,
    source_ref,
    tokens_ref,
    gate_ref,
    up_ref,
    slow_ref,
    prev_ref,
    slow_out,
    velocity_out,
    mate_slow,
    mate_prev,
    gate_w,
    up_w,
    slow_w,
    pair_w,
    act,
    out,
    upstream,
    grad,
    spread_in_0,
    spread_in_1,
    spread_out_0,
    spread_out_1,
    gossip_in_0,
    gossip_in_1,
    gossip_out_0,
    gossip_out_1,
    velocity,
    inv_rms,
    gate_act,
    up_act,
    hidden,
    load_sem,
    store_sem,
    token_send,
    token_recv,
    first_send,
    first_recv,
    second_send,
    second_recv,
    gossip_send,
    gossip_recv,
):
    mate = (mate_slow, mate_prev)
    spread_in = (spread_in_0, spread_in_1)
    spread_out = (spread_out_0, spread_out_1)
    gossip_in = (gossip_in_0, gossip_in_1)
    gossip_out = (gossip_out_0, gossip_out_1)
    section = lax.axis_index("section")
    replica = lax.axis_index("replica")
    rows, features = act.shape
    units = pair_w.shape[1]
    across = features // spread_in_0.shape[2]
    down = replicas // across

    def load(ref, target, index):
        return pltpu.make_async_copy(ref, target, load_sem.at[index])

    loads = (
        load(slow_ref, slow_w, 0),
        load(prev_ref, pair_w.at[1], 1),
        load(gate_ref, gate_w, 2),
        load(up_ref, up_w, 3),
    )
    for copy in loads:
        copy.start()

    barrier = pltpu.get_barrier_semaphore()

    def greet(target):
        def one(step, carry):
            pl.semaphore_signal(
                barrier,
                inc=1,
                device_id=(target, lax.rem(replica + step, replicas)),
                device_id_type=MESH,
            )
            return carry

        lax.fori_loop(0, replicas, one, 0)

    for target in range(sections):

        @pl.when(section != target)
        def _():
            greet(target)

    def greet_own(step, carry):
        pl.semaphore_signal(
            barrier,
            inc=1,
            device_id=(section, lax.rem(replica + step, replicas)),
            device_id_type=MESH,
        )
        return carry

    lax.fori_loop(1, replicas, greet_own, 0)
    pl.semaphore_wait(barrier, sections * replicas - 1)

    band = rows // sections

    def token_copy(origin):
        return pltpu.make_async_remote_copy(
            src_ref=tokens_ref,
            dst_ref=act.at[pl.ds(pl.multiple_of(origin * band, band), band)],
            send_sem=token_send,
            recv_sem=token_recv,
            device_id=(0, replica),
            device_id_type=MESH,
        )

    @pl.when(section != 0)
    def _():
        token_copy(section).start()

    @pl.when(section == 0)
    def _():
        pltpu.make_async_copy(tokens_ref, act.at[pl.ds(0, band)], token_recv).start()

    def area(ref, index):
        tall, wide = ref.shape[0] // down, ref.shape[1] // across
        top = pl.multiple_of(lax.div(index, across) * tall, tall)
        left = pl.multiple_of(lax.rem(index, across) * wide, wide)
        return ref.at[pl.ds(top, tall), pl.ds(left, wide)]

    def other(step):
        return lax.rem(replica + step * stride, replicas)

    def turn(position, index, length):
        ahead = lax.div(index + 1, 2) * (1 - 2 * lax.rem(index, 2))
        return lax.rem(position + length // 2 + ahead, length)

    def far_first(step):
        width, depth, height = torus
        x = turn(lax.div(replica, depth * height), lax.rem(lax.div(step, height), width), width)
        z = turn(lax.rem(lax.div(replica, height), depth), lax.div(step, height * width), depth)
        y = turn(lax.rem(replica, height), lax.rem(step, height), height)
        return (x * depth + z) * height + y

    def spread(ref, target, way):
        def one(step, carry):
            peer = far_first(step)
            pltpu.make_async_remote_copy(
                src_ref=area(ref, peer),
                dst_ref=spread_in[way].at[replica],
                send_sem=first_send.at[way],
                recv_sem=first_recv.at[way],
                device_id=(target, peer),
                device_id_type=MESH,
            ).start()
            return carry

        lax.fori_loop(0, replicas, one, 0)

    def spread_done(ref, way):
        pltpu.make_async_copy(ref, ref, first_send.at[way]).wait()

    def gather(ref, table, way):
        pltpu.make_async_copy(
            spread_in[way], spread_in[way], first_recv.at[way]
        ).wait()

        def pick(step, carry):
            spread_out[way][step] = spread_in[way][source_ref[table, step]]
            return carry

        lax.fori_loop(0, replicas, pick, 0, unroll=8)
        pltpu.make_async_copy(
            spread_out[way].at[replica], area(ref, replica), second_recv.at[way]
        ).start()

        def one(step, carry):
            peer = far_first(step)
            pltpu.make_async_remote_copy(
                src_ref=spread_out[way].at[peer],
                dst_ref=area(ref, replica),
                send_sem=second_send.at[way],
                recv_sem=second_recv.at[way],
                device_id=(section, peer),
                device_id_type=MESH,
            ).start()
            return carry

        lax.fori_loop(0, replicas - 1, one, 0)
        pltpu.make_async_copy(ref, ref, second_recv.at[way]).wait()

    def gather_done(way):
        part = spread_out[way].at[pl.ds(0, replicas - 1)]
        pltpu.make_async_copy(part, part, second_send.at[way]).wait()

    def gossip_first(part):
        pltpu.make_async_copy(
            area(pair_w.at[part], replica),
            gossip_in[part].at[replica],
            gossip_recv.at[part],
        ).start()

        def one(step, carry):
            peer = other(step)
            pltpu.make_async_remote_copy(
                src_ref=area(pair_w.at[part], peer),
                dst_ref=gossip_in[part].at[replica],
                send_sem=gossip_send.at[part],
                recv_sem=gossip_recv.at[part],
                device_id=(section, peer),
                device_id_type=MESH,
            ).start()
            return carry

        lax.fori_loop(1, replicas, one, 0)

    def gossip_second(part):
        pltpu.make_async_copy(
            gossip_in[part], gossip_in[part], gossip_recv.at[part]
        ).wait()

        def pick(step, carry):
            gossip_out[part][step] = gossip_in[part][source_ref[2 * sections - 2, step]]
            return carry

        lax.fori_loop(0, replicas, pick, 0, unroll=4)
        pltpu.make_async_copy(
            gossip_out[part].at[replica],
            area(mate[part], replica),
            gossip_recv.at[2 + part],
        ).start()

        def one(step, carry):
            peer = other(step)
            pltpu.make_async_remote_copy(
                src_ref=gossip_out[part].at[peer],
                dst_ref=area(mate[part], replica),
                send_sem=gossip_send.at[2 + part],
                recv_sem=gossip_recv.at[2 + part],
                device_id=(section, peer),
                device_id_type=MESH,
            ).start()
            return carry

        lax.fori_loop(1, replicas, one, 0)

    def gossip_done(part):
        for stage in range(2):
            piece = gossip_out[part].at[pl.ds(0, replicas - 1)]
            pltpu.make_async_copy(piece, piece, gossip_send.at[2 * stage + part]).wait()

    loads[0].wait()
    pair_w[0] = slow_w[...].astype(BF16)
    loads[1].wait()

    @pl.when(section >= sections // 2)
    def _():
        gossip_first(0)
        gossip_first(1)

    loads[2].wait()
    loads[3].wait()

    @pl.when(section == 0)
    def _():
        pltpu.make_async_copy(act, act, token_recv).wait()

    @pl.when(section > 0)
    def _():
        gather(act, section - 1, 0)

    wide = act[...].astype(F32)
    scale = lax.rsqrt(jnp.mean(wide * wide, axis=-1, keepdims=True) + EPSILON)
    inv_rms[...] = scale
    normed = (wide * scale).astype(BF16)
    gate = dot(normed, gate_w[...], NN)
    up = dot(normed, up_w[...], NN)
    gate_act[...] = gate
    up_act[...] = up
    hid = (jax.nn.silu(gate) * up).astype(BF16)
    hidden[...] = hid
    result = (act[...].astype(F32) + dot(hid, pair_w[0], NN)).astype(BF16)
    out[...] = result

    @pl.when(section < sections - 1)
    def _():
        spread(out, section + 1, 0)

    @pl.when(section == sections - 1)
    def _():
        upstream[...] = (out[...].astype(F32) / float(rows)).astype(BF16)

    @pl.when(section < sections // 2)
    def _():
        gossip_first(0)
        gossip_first(1)
        gossip_second(0)

    @pl.when(section < sections - 1)
    def _():
        gather(upstream, sections - 1 + section, 1)

    @pl.when(section > 0)
    def _():
        hidden_grad = dot(upstream[...], pair_w[0], NT)
        gate = gate_act[...]
        sig = jax.nn.sigmoid(gate)
        gate_grad = (hidden_grad * up_act[...] * sig * (1.0 + gate * (1.0 - sig))).astype(BF16)
        up_grad = (hidden_grad * gate * sig).astype(BF16)
        normed_grad = dot(gate_grad, gate_w[...], NT) + dot(up_grad, up_w[...], NT)
        scale = inv_rms[...]
        wide = act[...].astype(F32)
        mean = jnp.mean(normed_grad * wide, axis=-1, keepdims=True)
        grad[...] = (
            upstream[...].astype(F32) + scale * normed_grad - wide * scale**3 * mean
        ).astype(BF16)
        spread(grad, section - 1, 1)

    @pl.when(section >= sections // 2)
    def _():
        gossip_second(0)

    gossip_second(1)

    weight_grad = dot(hidden[...], upstream[...], TN)
    speed = (0.5 * MOMENTUM) * pair_w[1].astype(F32) + weight_grad
    velocity[...] = speed
    slow_w[...] = 0.5 * slow_w[...] - OUTER_RATE * (weight_grad + MOMENTUM * speed)
    stores = (
        pltpu.make_async_copy(slow_w, slow_out, store_sem.at[0]),
        pltpu.make_async_copy(velocity, velocity_out, store_sem.at[1]),
    )
    for copy in stores:
        copy.start()

    @pl.when(section != 0)
    def _():
        pltpu.make_async_copy(tokens_ref, tokens_ref, token_send).wait()
        gather_done(0)
        spread_done(grad, 1)

    @pl.when(section < sections - 1)
    def _():
        spread_done(out, 0)
        gather_done(1)

    for part in range(2):
        pltpu.make_async_copy(mate[part], mate[part], gossip_recv.at[2 + part]).wait()
        gossip_done(part)
    for copy in stores:
        copy.wait()


def local(sections, replicas, tokens, gate_weight, up_weight, slow_down, prev_outer, route, partner):
    rows = tokens.shape[1] * sections
    features = tokens.shape[2]
    units = gate_weight.shape[3]
    order = jnp.arange(replicas, dtype=jnp.int32)
    targets = route[:, 0]
    origins = jnp.sum(
        jnp.where(targets[:, :, None] == order, order[:, None], 0), axis=1, dtype=jnp.int32
    )
    sources = jnp.concatenate([origins, targets, partner[None]], axis=0)
    across = min(16, replicas)
    down = replicas // across
    piece = (rows // down, features // across)
    share = (units // down, features // across)
    stride = 37 if replicas == 64 else 1
    torus = (4, 8, 2) if replicas == 64 else (1, replicas, 1)
    anywhere = pl.BlockSpec(memory_space=pl.ANY)
    dma = pltpu.SemaphoreType.DMA
    slow, velocity, mate_slow, mate_prev = pl.pallas_call(
        functools.partial(kernel, sections, replicas, stride, torus),
        out_shape=(
            jax.ShapeDtypeStruct((units, features), F32),
            jax.ShapeDtypeStruct((units, features), F32),
            jax.ShapeDtypeStruct((units, features), BF16),
            jax.ShapeDtypeStruct((units, features), BF16),
        ),
        in_specs=[pl.BlockSpec(memory_space=pltpu.SMEM)] + [anywhere] * 5,
        out_specs=(anywhere,) * 4,
        scratch_shapes=[
            pltpu.VMEM((features, units), BF16),
            pltpu.VMEM((features, units), BF16),
            pltpu.VMEM((units, features), F32),
            pltpu.VMEM((2, units, features), BF16),
            pltpu.VMEM((rows, features), BF16),
            pltpu.VMEM((rows, features), BF16),
            pltpu.VMEM((rows, features), BF16),
            pltpu.VMEM((rows, features), BF16),
            pltpu.VMEM((replicas, *piece), BF16),
            pltpu.VMEM((replicas, *piece), BF16),
            pltpu.VMEM((replicas, *piece), BF16),
            pltpu.VMEM((replicas, *piece), BF16),
            pltpu.VMEM((replicas, *share), BF16),
            pltpu.VMEM((replicas, *share), BF16),
            pltpu.VMEM((replicas, *share), BF16),
            pltpu.VMEM((replicas, *share), BF16),
            pltpu.VMEM((units, features), F32),
            pltpu.VMEM((rows, 1), F32),
            pltpu.VMEM((rows, units), F32),
            pltpu.VMEM((rows, units), F32),
            pltpu.VMEM((rows, units), BF16),
            dma((4,)),
            dma((2,)),
            dma,
            dma,
            dma((2,)),
            dma((2,)),
            dma((2,)),
            dma((2,)),
            dma((4,)),
            dma((4,)),
        ],
        compiler_params=pltpu.CompilerParams(
            collective_id=0, has_side_effects=True, vmem_limit_bytes=60 * 2**20
        ),
        name="relay",
    )(sources, tokens[0], gate_weight[0, 0], up_weight[0, 0], slow_down[0, 0], prev_outer[0, 0])
    theirs = (0.5 * MOMENTUM) * mate_prev.astype(F32)
    new_slow = slow + (0.5 * mate_slow.astype(F32) - (OUTER_RATE * MOMENTUM) * theirs)
    new_outer = (velocity + theirs).astype(BF16)
    return (new_slow[None, None], new_outer[None, None])


def solution(mesh):
    sections, replicas = mesh.shape["section"], mesh.shape["replica"]
    own = P("section", "replica", None, None)
    return jax.shard_map(
        functools.partial(local, sections, replicas),
        mesh=mesh,
        in_specs=(P("replica", "section", None), own, own, own, own, P(), P()),
        out_specs=(own, own),
        check_vma=False,
    )
```

```python
import functools

import jax
import jax.numpy as jnp
from jax import lax
from jax.experimental import pallas as pl
from jax.experimental.pallas import tpu as pltpu
from jax.sharding import PartitionSpec as P

EPSILON = 1e-05
OUTER_RATE = 0.7
MOMENTUM = 0.9

MESH = pl.DeviceIdType.MESH
F32 = jnp.float32
BF16 = jnp.bfloat16

NN = (((1,), (0,)), ((), ()))
NT = (((1,), (1,)), ((), ()))
TN = (((0,), (0,)), ((), ()))


def dot(a, b, dims):
    return lax.dot_general(a, b, dims, preferred_element_type=F32)


def kernel(
    sections,
    replicas,
    stride,
    torus,
    origin_ref,
    target_ref,
    partner_ref,
    tokens_ref,
    gate_ref,
    up_ref,
    slow_ref,
    prev_ref,
    slow_out,
    velocity_out,
    mate_slow,
    mate_prev,
    gate_w,
    up_w,
    slow_w,
    pair_w,
    act,
    out,
    upstream,
    grad,
    spread_in_0,
    spread_in_1,
    spread_out_0,
    spread_out_1,
    gossip_in_0,
    gossip_in_1,
    gossip_in_2,
    gossip_in_3,
    gossip_out_0,
    gossip_out_1,
    gossip_out_2,
    gossip_out_3,
    velocity,
    inv_rms,
    gate_act,
    up_act,
    hidden,
    load_sem,
    store_sem,
    token_send,
    token_recv,
    first_send,
    first_recv,
    second_send,
    second_recv,
    gossip_send,
    gossip_recv,
    mate_send,
    mate_recv,
    gate_sem,
):
    mate = (mate_slow, mate_prev)
    spread_in = (spread_in_0, spread_in_1)
    spread_out = (spread_out_0, spread_out_1)
    gossip_in = (gossip_in_0, gossip_in_1, gossip_in_2, gossip_in_3)
    gossip_out = (gossip_out_0, gossip_out_1, gossip_out_2, gossip_out_3)
    section = lax.axis_index("section")
    replica = lax.axis_index("replica")
    rows, features = act.shape
    units = pair_w.shape[1]
    across = features // spread_in_0.shape[2]
    down = replicas // across

    def load(ref, target, index):
        return pltpu.make_async_copy(ref, target, load_sem.at[index])

    loads = (
        load(slow_ref, slow_w, 0),
        load(prev_ref, pair_w.at[1], 1),
        load(gate_ref, gate_w, 2),
        load(up_ref, up_w, 3),
    )
    for copy in loads:
        copy.start()

    barrier = pltpu.get_barrier_semaphore()

    def greet(target):
        def one(step, carry):
            pl.semaphore_signal(
                barrier,
                inc=1,
                device_id=(target, lax.rem(replica + step, replicas)),
                device_id_type=MESH,
            )
            return carry

        lax.fori_loop(0, replicas, one, 0)

    for target in range(sections):

        @pl.when(section != target)
        def _():
            greet(target)

    def greet_own(step, carry):
        pl.semaphore_signal(
            barrier,
            inc=1,
            device_id=(section, lax.rem(replica + step, replicas)),
            device_id_type=MESH,
        )
        return carry

    lax.fori_loop(1, replicas, greet_own, 0)
    pl.semaphore_wait(barrier, sections * replicas - 1)

    band = rows // sections

    def token_copy(origin):
        return pltpu.make_async_remote_copy(
            src_ref=tokens_ref,
            dst_ref=act.at[pl.ds(pl.multiple_of(origin * band, band), band)],
            send_sem=token_send,
            recv_sem=token_recv,
            device_id=(0, replica),
            device_id_type=MESH,
        )

    @pl.when(section != 0)
    def _():
        token_copy(section).start()

    @pl.when(section == 0)
    def _():
        pltpu.make_async_copy(tokens_ref, act.at[pl.ds(0, band)], token_recv).start()

    def area(ref, index):
        tall, wide = ref.shape[0] // down, ref.shape[1] // across
        top = pl.multiple_of(lax.div(index, across) * tall, tall)
        left = pl.multiple_of(lax.rem(index, across) * wide, wide)
        return ref.at[pl.ds(top, tall), pl.ds(left, wide)]

    def other(step):
        return lax.rem(replica + step * stride, replicas)

    def turn(position, index, length):
        ahead = lax.div(index + 1, 2) * (1 - 2 * lax.rem(index, 2))
        return lax.rem(position + length // 2 + ahead, length)

    def far_first(step):
        width, depth, height = torus
        x = turn(lax.div(replica, depth * height), lax.rem(lax.div(step, height), width), width)
        z = turn(lax.rem(lax.div(replica, height), depth), lax.div(step, height * width), depth)
        y = turn(lax.rem(replica, height), lax.rem(step, height), height)
        return (x * depth + z) * height + y

    def spread(ref, target, way):
        def one(step, carry):
            peer = far_first(step)
            pltpu.make_async_remote_copy(
                src_ref=area(ref, peer),
                dst_ref=spread_in[way].at[replica],
                send_sem=first_send.at[way],
                recv_sem=first_recv.at[way],
                device_id=(target, peer),
                device_id_type=MESH,
            ).start()
            return carry

        lax.fori_loop(0, replicas, one, 0)

    def spread_done(ref, way):
        pltpu.make_async_copy(ref, ref, first_send.at[way]).wait()

    def gather(ref, table, row, way):
        pltpu.make_async_copy(
            spread_in[way], spread_in[way], first_recv.at[way]
        ).wait()

        def pick(step, carry):
            spread_out[way][step] = spread_in[way][table[row, step]]
            return carry

        lax.fori_loop(0, replicas, pick, 0, unroll=8)
        pltpu.make_async_copy(
            spread_out[way].at[replica], area(ref, replica), second_recv.at[way]
        ).start()

        def one(step, carry):
            peer = far_first(step)
            pltpu.make_async_remote_copy(
                src_ref=spread_out[way].at[peer],
                dst_ref=area(ref, replica),
                send_sem=second_send.at[way],
                recv_sem=second_recv.at[way],
                device_id=(section, peer),
                device_id_type=MESH,
            ).start()
            return carry

        lax.fori_loop(0, replicas - 1, one, 0)
        pltpu.make_async_copy(ref, ref, second_recv.at[way]).wait()

    def gather_done(way):
        part = spread_out[way].at[pl.ds(0, replicas - 1)]
        pltpu.make_async_copy(part, part, second_send.at[way]).wait()

    half = lax.div(section, 2)
    helper = half * (sections - 1)
    helping = section == helper

    def gossip_first(part):
        for origin in range(2):
            landing = gossip_in[2 * origin + part]

            @pl.when(lax.rem(section, 2) == origin)
            def _():
                @pl.when(helping)
                def _():
                    pltpu.make_async_copy(
                        area(pair_w.at[part], replica),
                        landing.at[replica],
                        gossip_recv.at[2 * origin + part],
                    ).start()

                def one(step, carry):
                    peer = other(step)
                    pltpu.make_async_remote_copy(
                        src_ref=area(pair_w.at[part], peer),
                        dst_ref=landing.at[replica],
                        send_sem=gossip_send.at[part],
                        recv_sem=gossip_recv.at[2 * origin + part],
                        device_id=(helper, peer),
                        device_id_type=MESH,
                    ).start()
                    return carry

                lax.fori_loop(jnp.where(helping, 1, 0), replicas, one, 0)

    def gossip_second(origin, part):
        arrived, leaving = gossip_in[2 * origin + part], gossip_out[2 * origin + part]
        target = 2 * half + origin
        pltpu.make_async_copy(arrived, arrived, gossip_recv.at[2 * origin + part]).wait()

        def pick(step, carry):
            leaving[step] = arrived[partner_ref[step]]
            return carry

        lax.fori_loop(0, replicas, pick, 0, unroll=4)

        @pl.when(target == section)
        def _():
            pltpu.make_async_copy(
                leaving.at[replica], area(mate[part], replica), mate_recv.at[part]
            ).start()

        def one(step, carry):
            peer = other(step)
            pltpu.make_async_remote_copy(
                src_ref=leaving.at[peer],
                dst_ref=area(mate[part], replica),
                send_sem=mate_send.at[2 * origin + part],
                recv_sem=mate_recv.at[part],
                device_id=(target, peer),
                device_id_type=MESH,
            ).start()
            return carry

        lax.fori_loop(jnp.where(target == section, 1, 0), replicas, one, 0)

    def sent(sem, alone):
        whole, most = gossip_out[0], gossip_out[0].at[pl.ds(0, replicas - 1)]

        @pl.when(alone)
        def _():
            pltpu.make_async_copy(most, most, sem).wait()

        @pl.when(jnp.logical_not(alone))
        def _():
            pltpu.make_async_copy(whole, whole, sem).wait()

    def gossip_done():
        for part in range(2):
            sent(gossip_send.at[part], helping)

        @pl.when(helping)
        def _():
            for origin in range(2):
                for part in range(2):
                    sent(mate_send.at[2 * origin + part], 2 * half + origin == section)

    loads[0].wait()
    pair_w[0] = slow_w[...].astype(BF16)
    loads[1].wait()

    @pl.when(section >= sections // 2)
    def _():
        gossip_first(0)

    @pl.when(section == sections - 1)
    def _():
        gossip_first(1)

    loads[2].wait()
    loads[3].wait()

    @pl.when(section == 0)
    def _():
        pltpu.make_async_copy(act, act, token_recv).wait()

    @pl.when(section > 0)
    def _():
        gather(act, origin_ref, section - 1, 0)

    wide = act[...].astype(F32)
    scale = lax.rsqrt(jnp.mean(wide * wide, axis=-1, keepdims=True) + EPSILON)
    inv_rms[...] = scale
    normed = (wide * scale).astype(BF16)
    gate = dot(normed, gate_w[...], NN)
    up = dot(normed, up_w[...], NN)
    gate_act[...] = gate
    up_act[...] = up
    hid = (jax.nn.silu(gate) * up).astype(BF16)
    hidden[...] = hid
    result = (act[...].astype(F32) + dot(hid, pair_w[0], NN)).astype(BF16)
    out[...] = result

    @pl.when(section < sections - 1)
    def _():
        spread(out, section + 1, 0)

    @pl.when(section == sections - 1)
    def _():
        upstream[...] = (out[...].astype(F32) / float(rows)).astype(BF16)

    @pl.when(section == 1)
    def _():
        spread_done(out, 0)
        pl.semaphore_signal(gate_sem, inc=1, device_id=(0, replica), device_id_type=MESH)
        gossip_first(0)

    @pl.when((section > 0) & (section < sections - 1))
    def _():
        gossip_first(1)

    @pl.when(section == 0)
    def _():
        gossip_first(0)
        pl.semaphore_wait(gate_sem, 1)
        gossip_first(1)
        for part in range(2):
            for origin in range(2):
                gossip_second(origin, part)

    @pl.when(section < sections - 1)
    def _():
        gather(upstream, target_ref, section, 1)

    @pl.when(section > 0)
    def _():
        hidden_grad = dot(upstream[...], pair_w[0], NT)
        gate = gate_act[...]
        sig = jax.nn.sigmoid(gate)
        gate_grad = (hidden_grad * up_act[...] * sig * (1.0 + gate * (1.0 - sig))).astype(BF16)
        up_grad = (hidden_grad * gate * sig).astype(BF16)
        normed_grad = dot(gate_grad, gate_w[...], NT) + dot(up_grad, up_w[...], NT)
        scale = inv_rms[...]
        wide = act[...].astype(F32)
        mean = jnp.mean(normed_grad * wide, axis=-1, keepdims=True)
        grad[...] = (
            upstream[...].astype(F32) + scale * normed_grad - wide * scale**3 * mean
        ).astype(BF16)
        spread(grad, section - 1, 1)

    @pl.when(section == sections - 1)
    def _():
        for part in range(2):
            for origin in range(2):
                gossip_second(origin, part)

    weight_grad = dot(hidden[...], upstream[...], TN)
    speed = (0.5 * MOMENTUM) * pair_w[1].astype(F32) + weight_grad
    velocity[...] = speed
    slow_w[...] = 0.5 * slow_w[...] - OUTER_RATE * (weight_grad + MOMENTUM * speed)
    stores = (
        pltpu.make_async_copy(slow_w, slow_out, store_sem.at[0]),
        pltpu.make_async_copy(velocity, velocity_out, store_sem.at[1]),
    )
    for copy in stores:
        copy.start()

    @pl.when(section != 0)
    def _():
        pltpu.make_async_copy(tokens_ref, tokens_ref, token_send).wait()
        gather_done(0)
        spread_done(grad, 1)

    @pl.when((section < sections - 1) & (section != 1))
    def _():
        spread_done(out, 0)

    @pl.when(section < sections - 1)
    def _():
        gather_done(1)

    for part in range(2):
        pltpu.make_async_copy(mate[part], mate[part], mate_recv.at[part]).wait()
    gossip_done()
    for copy in stores:
        copy.wait()


def local(sections, replicas, tokens, gate_weight, up_weight, slow_down, prev_outer, route, partner):
    rows = tokens.shape[1] * sections
    features = tokens.shape[2]
    units = gate_weight.shape[3]
    order = jnp.arange(replicas, dtype=jnp.int32)
    targets = route[:, 0]
    origins = jnp.sum(
        jnp.where(targets[:, :, None] == order, order[:, None], 0), axis=1, dtype=jnp.int32
    )
    across = min(16, replicas)
    down = replicas // across
    piece = (rows // down, features // across)
    share = (units // down, features // across)
    stride = 37 if replicas == 64 else 1
    torus = (4, 8, 2) if replicas == 64 else (1, replicas, 1)
    anywhere = pl.BlockSpec(memory_space=pl.ANY)
    dma = pltpu.SemaphoreType.DMA
    slow, velocity, mate_slow, mate_prev = pl.pallas_call(
        functools.partial(kernel, sections, replicas, stride, torus),
        out_shape=(
            jax.ShapeDtypeStruct((units, features), F32),
            jax.ShapeDtypeStruct((units, features), F32),
            jax.ShapeDtypeStruct((units, features), BF16),
            jax.ShapeDtypeStruct((units, features), BF16),
        ),
        in_specs=[pl.BlockSpec(memory_space=pltpu.SMEM)] * 3 + [pl.BlockSpec(memory_space=pltpu.HBM)] * 5,
        out_specs=(anywhere,) * 4,
        scratch_shapes=[
            pltpu.VMEM((features, units), BF16),
            pltpu.VMEM((features, units), BF16),
            pltpu.VMEM((units, features), F32),
            pltpu.VMEM((2, units, features), BF16),
            pltpu.VMEM((rows, features), BF16),
            pltpu.VMEM((rows, features), BF16),
            pltpu.VMEM((rows, features), BF16),
            pltpu.VMEM((rows, features), BF16),
            pltpu.VMEM((replicas, *piece), BF16),
            pltpu.VMEM((replicas, *piece), BF16),
            pltpu.VMEM((replicas, *piece), BF16),
            pltpu.VMEM((replicas, *piece), BF16),
            pltpu.VMEM((replicas, *share), BF16),
            pltpu.VMEM((replicas, *share), BF16),
            pltpu.VMEM((replicas, *share), BF16),
            pltpu.VMEM((replicas, *share), BF16),
            pltpu.VMEM((replicas, *share), BF16),
            pltpu.VMEM((replicas, *share), BF16),
            pltpu.VMEM((replicas, *share), BF16),
            pltpu.VMEM((replicas, *share), BF16),
            pltpu.VMEM((units, features), F32),
            pltpu.VMEM((rows, 1), F32),
            pltpu.VMEM((rows, units), F32),
            pltpu.VMEM((rows, units), F32),
            pltpu.VMEM((rows, units), BF16),
            dma((4,)),
            dma((2,)),
            dma,
            dma,
            dma((2,)),
            dma((2,)),
            dma((2,)),
            dma((2,)),
            dma((2,)),
            dma((4,)),
            dma((4,)),
            dma((2,)),
            pltpu.SemaphoreType.REGULAR,
        ],
        compiler_params=pltpu.CompilerParams(
            collective_id=0, has_side_effects=True, vmem_limit_bytes=40 * 2**20
        ),
        name="relay",
    )(
        origins,
        targets,
        partner,
        pltpu.with_memory_space_constraint(tokens[0], pltpu.HBM),
        pltpu.with_memory_space_constraint(gate_weight[0, 0], pltpu.HBM),
        pltpu.with_memory_space_constraint(up_weight[0, 0], pltpu.HBM),
        pltpu.with_memory_space_constraint(slow_down[0, 0], pltpu.HBM),
        pltpu.with_memory_space_constraint(prev_outer[0, 0], pltpu.HBM),
    )
    theirs = (0.5 * MOMENTUM) * mate_prev.astype(F32)
    new_slow = slow + (0.5 * mate_slow.astype(F32) - (OUTER_RATE * MOMENTUM) * theirs)
    new_outer = (velocity + theirs).astype(BF16)
    return (new_slow[None, None], new_outer[None, None])


def solution(mesh):
    sections, replicas = mesh.shape["section"], mesh.shape["replica"]
    own = P("section", "replica", None, None)
    return jax.shard_map(
        functools.partial(local, sections, replicas),
        mesh=mesh,
        in_specs=(P("replica", "section", None), own, own, own, own, P(), P()),
        out_specs=(own, own),
        check_vma=False,
    )
```

```python
import functools

import jax
import jax.numpy as jnp
from jax import lax
from jax.experimental import pallas as pl
from jax.experimental.pallas import tpu as pltpu
from jax.sharding import PartitionSpec as P

EPSILON = 1e-05
OUTER_RATE = 0.7
MOMENTUM = 0.9

MESH = pl.DeviceIdType.MESH
F32 = jnp.float32
BF16 = jnp.bfloat16

NN = (((1,), (0,)), ((), ()))
NT = (((1,), (1,)), ((), ()))
TN = (((0,), (0,)), ((), ()))


def dot(a, b, dims):
    return lax.dot_general(a, b, dims, preferred_element_type=F32)


def kernel(
    sections,
    replicas,
    stride,
    torus,
    origin_ref,
    target_ref,
    partner_ref,
    tokens_ref,
    gate_ref,
    up_ref,
    slow_ref,
    prev_ref,
    slow_out,
    velocity_out,
    mate_slow,
    mate_prev,
    gate_w,
    up_w,
    slow_w,
    pair_w,
    act,
    out,
    upstream,
    grad,
    spread_in_0,
    spread_in_1,
    spread_out_0,
    spread_out_1,
    gossip_in_0,
    gossip_in_1,
    gossip_in_2,
    gossip_in_3,
    gossip_out_0,
    gossip_out_1,
    gossip_out_2,
    gossip_out_3,
    velocity,
    inv_rms,
    gate_act,
    up_act,
    hidden,
    load_sem,
    store_sem,
    token_send,
    token_recv,
    first_send,
    first_recv,
    second_send,
    second_recv,
    gossip_send,
    gossip_recv,
    mate_send,
    mate_recv,
    gate_sem,
):
    mate = (mate_slow, mate_prev)
    spread_in = (spread_in_0, spread_in_1)
    spread_out = (spread_out_0, spread_out_1)
    gossip_in = (gossip_in_0, gossip_in_1, gossip_in_2, gossip_in_3)
    gossip_out = (gossip_out_0, gossip_out_1, gossip_out_2, gossip_out_3)
    section = lax.axis_index("section")
    replica = lax.axis_index("replica")
    rows, features = act.shape
    units = pair_w.shape[1]
    across = features // spread_in_0.shape[2]
    down = replicas // across

    def load(ref, target, index):
        return pltpu.make_async_copy(ref, target, load_sem.at[index])

    loads = (
        load(slow_ref, slow_w, 0),
        load(prev_ref, pair_w.at[1], 1),
        load(gate_ref, gate_w, 2),
        load(up_ref, up_w, 3),
    )
    for copy in loads:
        copy.start()

    barrier = pltpu.get_barrier_semaphore()

    def greet(target):
        def one(step, carry):
            pl.semaphore_signal(
                barrier,
                inc=1,
                device_id=(target, lax.rem(replica + step, replicas)),
                device_id_type=MESH,
            )
            return carry

        lax.fori_loop(0, replicas, one, 0)

    for target in range(sections):

        @pl.when(section != target)
        def _():
            greet(target)

    def greet_own(step, carry):
        pl.semaphore_signal(
            barrier,
            inc=1,
            device_id=(section, lax.rem(replica + step, replicas)),
            device_id_type=MESH,
        )
        return carry

    lax.fori_loop(1, replicas, greet_own, 0)
    pl.semaphore_wait(barrier, sections * replicas - 1)

    band = rows // sections

    def token_copy(origin):
        return pltpu.make_async_remote_copy(
            src_ref=tokens_ref,
            dst_ref=act.at[pl.ds(pl.multiple_of(origin * band, band), band)],
            send_sem=token_send,
            recv_sem=token_recv,
            device_id=(0, replica),
            device_id_type=MESH,
        )

    @pl.when(section != 0)
    def _():
        token_copy(section).start()

    @pl.when(section == 0)
    def _():
        pltpu.make_async_copy(tokens_ref, act.at[pl.ds(0, band)], token_recv).start()

    def area(ref, index):
        tall, wide = ref.shape[0] // down, ref.shape[1] // across
        top = pl.multiple_of(lax.div(index, across) * tall, tall)
        left = pl.multiple_of(lax.rem(index, across) * wide, wide)
        return ref.at[pl.ds(top, tall), pl.ds(left, wide)]

    def other(step):
        return lax.rem(replica + step * stride, replicas)

    def turn(position, index, length):
        ahead = lax.div(index + 1, 2) * (1 - 2 * lax.rem(index, 2))
        return lax.rem(position + length // 2 + ahead, length)

    def far_first(step):
        width, depth, height = torus
        x = turn(lax.div(replica, depth * height), lax.div(step, depth * height), width)
        z = turn(lax.rem(lax.div(replica, height), depth), lax.rem(step, depth), depth)
        y = turn(lax.rem(replica, height), lax.rem(lax.div(step, depth), height), height)
        return (x * depth + z) * height + y

    def spread(ref, target, way):
        def one(step, carry):
            peer = far_first(step)
            pltpu.make_async_remote_copy(
                src_ref=area(ref, peer),
                dst_ref=spread_in[way].at[replica],
                send_sem=first_send.at[way],
                recv_sem=first_recv.at[way],
                device_id=(target, peer),
                device_id_type=MESH,
            ).start()
            return carry

        lax.fori_loop(0, replicas, one, 0)

    def spread_done(ref, way):
        pltpu.make_async_copy(ref, ref, first_send.at[way]).wait()

    def gather(ref, table, row, way):
        pltpu.make_async_copy(
            spread_in[way], spread_in[way], first_recv.at[way]
        ).wait()

        def pick(step, carry):
            spread_out[way][step] = spread_in[way][table[row, step]]
            return carry

        lax.fori_loop(0, replicas, pick, 0, unroll=8)
        pltpu.make_async_copy(
            spread_out[way].at[replica], area(ref, replica), second_recv.at[way]
        ).start()

        def one(step, carry):
            peer = far_first(step)
            pltpu.make_async_remote_copy(
                src_ref=spread_out[way].at[peer],
                dst_ref=area(ref, replica),
                send_sem=second_send.at[way],
                recv_sem=second_recv.at[way],
                device_id=(section, peer),
                device_id_type=MESH,
            ).start()
            return carry

        lax.fori_loop(0, replicas - 1, one, 0)
        pltpu.make_async_copy(ref, ref, second_recv.at[way]).wait()

    def gather_done(way):
        part = spread_out[way].at[pl.ds(0, replicas - 1)]
        pltpu.make_async_copy(part, part, second_send.at[way]).wait()

    half = lax.div(section, 2)
    helper = half * (sections - 1)
    helping = section == helper

    def gossip_first(part):
        for origin in range(2):
            landing = gossip_in[2 * origin + part]

            @pl.when(lax.rem(section, 2) == origin)
            def _():
                @pl.when(helping)
                def _():
                    pltpu.make_async_copy(
                        area(pair_w.at[part], replica),
                        landing.at[replica],
                        gossip_recv.at[2 * origin + part],
                    ).start()

                def one(step, carry):
                    peer = other(step)
                    pltpu.make_async_remote_copy(
                        src_ref=area(pair_w.at[part], peer),
                        dst_ref=landing.at[replica],
                        send_sem=gossip_send.at[part],
                        recv_sem=gossip_recv.at[2 * origin + part],
                        device_id=(helper, peer),
                        device_id_type=MESH,
                    ).start()
                    return carry

                lax.fori_loop(jnp.where(helping, 1, 0), replicas, one, 0)

    def gossip_second(origin, part):
        arrived, leaving = gossip_in[2 * origin + part], gossip_out[2 * origin + part]
        target = 2 * half + origin
        pltpu.make_async_copy(arrived, arrived, gossip_recv.at[2 * origin + part]).wait()

        def pick(step, carry):
            leaving[step] = arrived[partner_ref[step]]
            return carry

        lax.fori_loop(0, replicas, pick, 0, unroll=4)

        @pl.when(target == section)
        def _():
            pltpu.make_async_copy(
                leaving.at[replica], area(mate[part], replica), mate_recv.at[part]
            ).start()

        def one(step, carry):
            peer = other(step)
            pltpu.make_async_remote_copy(
                src_ref=leaving.at[peer],
                dst_ref=area(mate[part], replica),
                send_sem=mate_send.at[2 * origin + part],
                recv_sem=mate_recv.at[part],
                device_id=(target, peer),
                device_id_type=MESH,
            ).start()
            return carry

        lax.fori_loop(jnp.where(target == section, 1, 0), replicas, one, 0)

    def sent(sem, alone):
        whole, most = gossip_out[0], gossip_out[0].at[pl.ds(0, replicas - 1)]

        @pl.when(alone)
        def _():
            pltpu.make_async_copy(most, most, sem).wait()

        @pl.when(jnp.logical_not(alone))
        def _():
            pltpu.make_async_copy(whole, whole, sem).wait()

    def gossip_done():
        for part in range(2):
            sent(gossip_send.at[part], helping)

        @pl.when(helping)
        def _():
            for origin in range(2):
                for part in range(2):
                    sent(mate_send.at[2 * origin + part], 2 * half + origin == section)

    loads[0].wait()
    pair_w[0] = slow_w[...].astype(BF16)
    loads[1].wait()

    @pl.when(section >= sections // 2)
    def _():
        gossip_first(0)

    @pl.when(section == sections - 1)
    def _():
        gossip_first(1)

    loads[2].wait()
    loads[3].wait()

    @pl.when(section == 0)
    def _():
        pltpu.make_async_copy(act, act, token_recv).wait()

    @pl.when(section > 0)
    def _():
        gather(act, origin_ref, section - 1, 0)

    wide = act[...].astype(F32)
    scale = lax.rsqrt(jnp.mean(wide * wide, axis=-1, keepdims=True) + EPSILON)
    inv_rms[...] = scale
    normed = (wide * scale).astype(BF16)
    gate = dot(normed, gate_w[...], NN)
    up = dot(normed, up_w[...], NN)
    gate_act[...] = gate
    up_act[...] = up
    hid = (jax.nn.silu(gate) * up).astype(BF16)
    hidden[...] = hid
    result = (act[...].astype(F32) + dot(hid, pair_w[0], NN)).astype(BF16)
    out[...] = result

    @pl.when(section < sections - 1)
    def _():
        spread(out, section + 1, 0)

    @pl.when(section == sections - 1)
    def _():
        upstream[...] = (out[...].astype(F32) / float(rows)).astype(BF16)

    @pl.when(section == 1)
    def _():
        spread_done(out, 0)
        pl.semaphore_signal(gate_sem, inc=1, device_id=(0, replica), device_id_type=MESH)
        gossip_first(0)

    @pl.when((section > 0) & (section < sections - 1))
    def _():
        gossip_first(1)

    @pl.when(section == 0)
    def _():
        gossip_first(0)
        pl.semaphore_wait(gate_sem, 1)
        gossip_first(1)
        for part in range(2):
            for origin in range(2):
                gossip_second(origin, part)

    @pl.when(section < sections - 1)
    def _():
        gather(upstream, target_ref, section, 1)

    @pl.when(section > 0)
    def _():
        hidden_grad = dot(upstream[...], pair_w[0], NT)
        gate = gate_act[...]
        sig = jax.nn.sigmoid(gate)
        gate_grad = (hidden_grad * up_act[...] * sig * (1.0 + gate * (1.0 - sig))).astype(BF16)
        up_grad = (hidden_grad * gate * sig).astype(BF16)
        normed_grad = dot(gate_grad, gate_w[...], NT) + dot(up_grad, up_w[...], NT)
        scale = inv_rms[...]
        wide = act[...].astype(F32)
        mean = jnp.mean(normed_grad * wide, axis=-1, keepdims=True)
        grad[...] = (
            upstream[...].astype(F32) + scale * normed_grad - wide * scale**3 * mean
        ).astype(BF16)
        spread(grad, section - 1, 1)

    @pl.when(section == sections - 1)
    def _():
        for part in range(2):
            for origin in range(2):
                gossip_second(origin, part)

    weight_grad = dot(hidden[...], upstream[...], TN)
    speed = (0.5 * MOMENTUM) * pair_w[1].astype(F32) + weight_grad
    velocity[...] = speed
    slow_w[...] = 0.5 * slow_w[...] - OUTER_RATE * (weight_grad + MOMENTUM * speed)
    stores = (
        pltpu.make_async_copy(slow_w, slow_out, store_sem.at[0]),
        pltpu.make_async_copy(velocity, velocity_out, store_sem.at[1]),
    )
    for copy in stores:
        copy.start()

    @pl.when(section != 0)
    def _():
        pltpu.make_async_copy(tokens_ref, tokens_ref, token_send).wait()
        gather_done(0)
        spread_done(grad, 1)

    @pl.when((section < sections - 1) & (section != 1))
    def _():
        spread_done(out, 0)

    @pl.when(section < sections - 1)
    def _():
        gather_done(1)

    for part in range(2):
        pltpu.make_async_copy(mate[part], mate[part], mate_recv.at[part]).wait()
    gossip_done()
    for copy in stores:
        copy.wait()


def local(sections, replicas, tokens, gate_weight, up_weight, slow_down, prev_outer, route, partner):
    rows = tokens.shape[1] * sections
    features = tokens.shape[2]
    units = gate_weight.shape[3]
    order = jnp.arange(replicas, dtype=jnp.int32)
    targets = route[:, 0]
    origins = jnp.sum(
        jnp.where(targets[:, :, None] == order, order[:, None], 0), axis=1, dtype=jnp.int32
    )
    across = min(16, replicas)
    down = replicas // across
    piece = (rows // down, features // across)
    share = (units // down, features // across)
    stride = 37 if replicas == 64 else 1
    torus = (4, 8, 2) if replicas == 64 else (1, replicas, 1)
    anywhere = pl.BlockSpec(memory_space=pl.ANY)
    dma = pltpu.SemaphoreType.DMA
    slow, velocity, mate_slow, mate_prev = pl.pallas_call(
        functools.partial(kernel, sections, replicas, stride, torus),
        out_shape=(
            jax.ShapeDtypeStruct((units, features), F32),
            jax.ShapeDtypeStruct((units, features), F32),
            jax.ShapeDtypeStruct((units, features), BF16),
            jax.ShapeDtypeStruct((units, features), BF16),
        ),
        in_specs=[pl.BlockSpec(memory_space=pltpu.SMEM)] * 3 + [pl.BlockSpec(memory_space=pltpu.HBM)] * 5,
        out_specs=(anywhere,) * 4,
        scratch_shapes=[
            pltpu.VMEM((features, units), BF16),
            pltpu.VMEM((features, units), BF16),
            pltpu.VMEM((units, features), F32),
            pltpu.VMEM((2, units, features), BF16),
            pltpu.VMEM((rows, features), BF16),
            pltpu.VMEM((rows, features), BF16),
            pltpu.VMEM((rows, features), BF16),
            pltpu.VMEM((rows, features), BF16),
            pltpu.VMEM((replicas, *piece), BF16),
            pltpu.VMEM((replicas, *piece), BF16),
            pltpu.VMEM((replicas, *piece), BF16),
            pltpu.VMEM((replicas, *piece), BF16),
            pltpu.VMEM((replicas, *share), BF16),
            pltpu.VMEM((replicas, *share), BF16),
            pltpu.VMEM((replicas, *share), BF16),
            pltpu.VMEM((replicas, *share), BF16),
            pltpu.VMEM((replicas, *share), BF16),
            pltpu.VMEM((replicas, *share), BF16),
            pltpu.VMEM((replicas, *share), BF16),
            pltpu.VMEM((replicas, *share), BF16),
            pltpu.VMEM((units, features), F32),
            pltpu.VMEM((rows, 1), F32),
            pltpu.VMEM((rows, units), F32),
            pltpu.VMEM((rows, units), F32),
            pltpu.VMEM((rows, units), BF16),
            dma((4,)),
            dma((2,)),
            dma,
            dma,
            dma((2,)),
            dma((2,)),
            dma((2,)),
            dma((2,)),
            dma((2,)),
            dma((4,)),
            dma((4,)),
            dma((2,)),
            pltpu.SemaphoreType.REGULAR,
        ],
        compiler_params=pltpu.CompilerParams(
            collective_id=0, has_side_effects=True, vmem_limit_bytes=40 * 2**20
        ),
        name="relay",
    )(
        origins,
        targets,
        partner,
        pltpu.with_memory_space_constraint(tokens[0], pltpu.HBM),
        pltpu.with_memory_space_constraint(gate_weight[0, 0], pltpu.HBM),
        pltpu.with_memory_space_constraint(up_weight[0, 0], pltpu.HBM),
        pltpu.with_memory_space_constraint(slow_down[0, 0], pltpu.HBM),
        pltpu.with_memory_space_constraint(prev_outer[0, 0], pltpu.HBM),
    )
    theirs = (0.5 * MOMENTUM) * mate_prev.astype(F32)
    new_slow = slow + (0.5 * mate_slow.astype(F32) - (OUTER_RATE * MOMENTUM) * theirs)
    new_outer = (velocity + theirs).astype(BF16)
    return (new_slow[None, None], new_outer[None, None])


def solution(mesh):
    sections, replicas = mesh.shape["section"], mesh.shape["replica"]
    own = P("section", "replica", None, None)
    return jax.shard_map(
        functools.partial(local, sections, replicas),
        mesh=mesh,
        in_specs=(P("replica", "section", None), own, own, own, own, P(), P()),
        out_specs=(own, own),
        check_vma=False,
    )
```

```python
import functools

import jax
import jax.numpy as jnp
from jax import lax
from jax.experimental import pallas as pl
from jax.experimental.pallas import tpu as pltpu
from jax.sharding import PartitionSpec as P

EPSILON = 1e-05
OUTER_RATE = 0.7
MOMENTUM = 0.9

MESH = pl.DeviceIdType.MESH
F32 = jnp.float32
BF16 = jnp.bfloat16

NN = (((1,), (0,)), ((), ()))
NT = (((1,), (1,)), ((), ()))
TN = (((0,), (0,)), ((), ()))


def dot(a, b, dims):
    return lax.dot_general(a, b, dims, preferred_element_type=F32)


def kernel(
    sections,
    replicas,
    stride,
    torus,
    origin_ref,
    target_ref,
    partner_ref,
    tokens_ref,
    gate_ref,
    up_ref,
    slow_ref,
    prev_ref,
    slow_out,
    velocity_out,
    mate_slow,
    mate_prev,
    gate_w,
    up_w,
    slow_w,
    pair_w,
    act,
    out,
    upstream,
    grad,
    spread_in_0,
    spread_in_1,
    spread_out_0,
    spread_out_1,
    gossip_in_0,
    gossip_in_1,
    gossip_in_2,
    gossip_in_3,
    gossip_out_0,
    gossip_out_1,
    gossip_out_2,
    gossip_out_3,
    velocity,
    inv_rms,
    gate_act,
    up_act,
    hidden,
    load_sem,
    store_sem,
    token_send,
    token_recv,
    first_send,
    first_recv,
    second_send,
    second_recv,
    gossip_send,
    gossip_recv,
    mate_send,
    mate_recv,
    gate_sem,
):
    mate = (mate_slow, mate_prev)
    spread_in = (spread_in_0, spread_in_1)
    spread_out = (spread_out_0, spread_out_1)
    gossip_in = (gossip_in_0, gossip_in_1, gossip_in_2, gossip_in_3)
    gossip_out = (gossip_out_0, gossip_out_1, gossip_out_2, gossip_out_3)
    section = lax.axis_index("section")
    replica = lax.axis_index("replica")
    rows, features = act.shape
    units = pair_w.shape[1]
    across = features // spread_in_0.shape[2]
    down = replicas // across

    def load(ref, target, index):
        return pltpu.make_async_copy(ref, target, load_sem.at[index])

    loads = (
        load(slow_ref, slow_w, 0),
        load(prev_ref, pair_w.at[1], 1),
        load(gate_ref, gate_w, 2),
        load(up_ref, up_w, 3),
    )
    for copy in loads:
        copy.start()

    barrier = pltpu.get_barrier_semaphore()

    def greet(target):
        def one(step, carry):
            pl.semaphore_signal(
                barrier,
                inc=1,
                device_id=(target, lax.rem(replica + step, replicas)),
                device_id_type=MESH,
            )
            return carry

        lax.fori_loop(0, replicas, one, 0, unroll=4)

    for target in range(sections):

        @pl.when(section != target)
        def _():
            greet(target)

    def greet_own(step, carry):
        pl.semaphore_signal(
            barrier,
            inc=1,
            device_id=(section, lax.rem(replica + step, replicas)),
            device_id_type=MESH,
        )
        return carry

    lax.fori_loop(1, replicas, greet_own, 0)
    pl.semaphore_wait(barrier, sections * replicas - 1)

    band = rows // sections

    def token_copy(origin):
        return pltpu.make_async_remote_copy(
            src_ref=tokens_ref,
            dst_ref=act.at[pl.ds(pl.multiple_of(origin * band, band), band)],
            send_sem=token_send,
            recv_sem=token_recv,
            device_id=(0, replica),
            device_id_type=MESH,
        )

    @pl.when(section != 0)
    def _():
        token_copy(section).start()

    @pl.when(section == 0)
    def _():
        pltpu.make_async_copy(tokens_ref, act.at[pl.ds(0, band)], token_recv).start()

    def area(ref, index):
        tall, wide = ref.shape[0] // down, ref.shape[1] // across
        top = pl.multiple_of(lax.div(index, across) * tall, tall)
        left = pl.multiple_of(lax.rem(index, across) * wide, wide)
        return ref.at[pl.ds(top, tall), pl.ds(left, wide)]

    def other(step):
        return lax.rem(replica + step * stride, replicas)

    def turn(position, index, length):
        ahead = lax.div(index + 1, 2) * (1 - 2 * lax.rem(index, 2))
        return lax.rem(position + length // 2 + ahead, length)

    def far_first(step):
        width, depth, height = torus
        x = turn(lax.div(replica, depth * height), lax.div(step, depth * height), width)
        z = turn(lax.rem(lax.div(replica, height), depth), lax.rem(step, depth), depth)
        y = turn(lax.rem(replica, height), lax.rem(lax.div(step, depth), height), height)
        return (x * depth + z) * height + y

    def spread(ref, target, way):
        def one(step, carry):
            peer = far_first(step)
            pltpu.make_async_remote_copy(
                src_ref=area(ref, peer),
                dst_ref=spread_in[way].at[replica],
                send_sem=first_send.at[way],
                recv_sem=first_recv.at[way],
                device_id=(target, peer),
                device_id_type=MESH,
            ).start()
            return carry

        lax.fori_loop(0, replicas, one, 0)

    def spread_done(ref, way):
        pltpu.make_async_copy(ref, ref, first_send.at[way]).wait()

    def gather(ref, table, row, way):
        pltpu.make_async_copy(
            spread_in[way], spread_in[way], first_recv.at[way]
        ).wait()

        def pick(step, carry):
            spread_out[way][step] = spread_in[way][table[row, step]]
            return carry

        lax.fori_loop(0, replicas, pick, 0, unroll=8)
        pltpu.make_async_copy(
            spread_out[way].at[replica], area(ref, replica), second_recv.at[way]
        ).start()

        def one(step, carry):
            peer = far_first(step)
            pltpu.make_async_remote_copy(
                src_ref=spread_out[way].at[peer],
                dst_ref=area(ref, replica),
                send_sem=second_send.at[way],
                recv_sem=second_recv.at[way],
                device_id=(section, peer),
                device_id_type=MESH,
            ).start()
            return carry

        lax.fori_loop(0, replicas - 1, one, 0)
        pltpu.make_async_copy(ref, ref, second_recv.at[way]).wait()

    def gather_done(way):
        part = spread_out[way].at[pl.ds(0, replicas - 1)]
        pltpu.make_async_copy(part, part, second_send.at[way]).wait()

    half = lax.div(section, 2)
    helper = half * (sections - 1)
    helping = section == helper

    def gossip_first(part):
        for origin in range(2):
            landing = gossip_in[2 * origin + part]

            @pl.when(lax.rem(section, 2) == origin)
            def _():
                @pl.when(helping)
                def _():
                    pltpu.make_async_copy(
                        area(pair_w.at[part], replica),
                        landing.at[replica],
                        gossip_recv.at[2 * origin + part],
                    ).start()

                def one(step, carry):
                    peer = other(step)
                    pltpu.make_async_remote_copy(
                        src_ref=area(pair_w.at[part], peer),
                        dst_ref=landing.at[replica],
                        send_sem=gossip_send.at[part],
                        recv_sem=gossip_recv.at[2 * origin + part],
                        device_id=(helper, peer),
                        device_id_type=MESH,
                    ).start()
                    return carry

                lax.fori_loop(jnp.where(helping, 1, 0), replicas, one, 0)

    def gossip_second(origin, part):
        arrived, leaving = gossip_in[2 * origin + part], gossip_out[2 * origin + part]
        target = 2 * half + origin
        pltpu.make_async_copy(arrived, arrived, gossip_recv.at[2 * origin + part]).wait()

        def pick(step, carry):
            leaving[step] = arrived[partner_ref[step]]
            return carry

        lax.fori_loop(0, replicas, pick, 0, unroll=4)

        @pl.when(target == section)
        def _():
            pltpu.make_async_copy(
                leaving.at[replica], area(mate[part], replica), mate_recv.at[part]
            ).start()

        def one(step, carry):
            peer = other(step)
            pltpu.make_async_remote_copy(
                src_ref=leaving.at[peer],
                dst_ref=area(mate[part], replica),
                send_sem=mate_send.at[2 * origin + part],
                recv_sem=mate_recv.at[part],
                device_id=(target, peer),
                device_id_type=MESH,
            ).start()
            return carry

        lax.fori_loop(jnp.where(target == section, 1, 0), replicas, one, 0)

    def sent(sem, alone):
        whole, most = gossip_out[0], gossip_out[0].at[pl.ds(0, replicas - 1)]

        @pl.when(alone)
        def _():
            pltpu.make_async_copy(most, most, sem).wait()

        @pl.when(jnp.logical_not(alone))
        def _():
            pltpu.make_async_copy(whole, whole, sem).wait()

    def gossip_done():
        for part in range(2):
            sent(gossip_send.at[part], helping)

        @pl.when(helping)
        def _():
            for origin in range(2):
                for part in range(2):
                    sent(mate_send.at[2 * origin + part], 2 * half + origin == section)

    loads[0].wait()
    pair_w[0] = slow_w[...].astype(BF16)
    loads[1].wait()

    @pl.when(section >= sections // 2)
    def _():
        gossip_first(0)

    @pl.when(section == sections - 1)
    def _():
        gossip_first(1)

    loads[2].wait()
    loads[3].wait()

    @pl.when(section == 0)
    def _():
        pltpu.make_async_copy(act, act, token_recv).wait()

    @pl.when(section > 0)
    def _():
        gather(act, origin_ref, section - 1, 0)

    wide = act[...].astype(F32)
    scale = lax.rsqrt(jnp.mean(wide * wide, axis=-1, keepdims=True) + EPSILON)
    inv_rms[...] = scale
    normed = (wide * scale).astype(BF16)
    gate = dot(normed, gate_w[...], NN)
    up = dot(normed, up_w[...], NN)
    gate_act[...] = gate
    up_act[...] = up
    hid = (jax.nn.silu(gate) * up).astype(BF16)
    hidden[...] = hid
    result = (act[...].astype(F32) + dot(hid, pair_w[0], NN)).astype(BF16)
    out[...] = result

    @pl.when(section < sections - 1)
    def _():
        spread(out, section + 1, 0)

    @pl.when(section == sections - 1)
    def _():
        upstream[...] = (out[...].astype(F32) / float(rows)).astype(BF16)

    @pl.when(section == 1)
    def _():
        spread_done(out, 0)
        pl.semaphore_signal(gate_sem, inc=1, device_id=(0, replica), device_id_type=MESH)
        gossip_first(0)

    @pl.when((section > 0) & (section < sections - 1))
    def _():
        gossip_first(1)

    @pl.when(section == 0)
    def _():
        gossip_first(0)
        pl.semaphore_wait(gate_sem, 1)
        gossip_first(1)
        for part in range(2):
            for origin in range(2):
                gossip_second(origin, part)

    @pl.when(section < sections - 1)
    def _():
        gather(upstream, target_ref, section, 1)

    @pl.when(section > 0)
    def _():
        hidden_grad = dot(upstream[...], pair_w[0], NT)
        gate = gate_act[...]
        sig = jax.nn.sigmoid(gate)
        gate_grad = (hidden_grad * up_act[...] * sig * (1.0 + gate * (1.0 - sig))).astype(BF16)
        up_grad = (hidden_grad * gate * sig).astype(BF16)
        normed_grad = dot(gate_grad, gate_w[...], NT) + dot(up_grad, up_w[...], NT)
        scale = inv_rms[...]
        wide = act[...].astype(F32)
        mean = jnp.mean(normed_grad * wide, axis=-1, keepdims=True)
        grad[...] = (
            upstream[...].astype(F32) + scale * normed_grad - wide * scale**3 * mean
        ).astype(BF16)
        spread(grad, section - 1, 1)

    @pl.when(section == sections - 1)
    def _():
        for part in range(2):
            for origin in range(2):
                gossip_second(origin, part)

    stores = []
    for block in range(units // 128):
        lines = pl.ds(block * 128, 128)
        weight_grad = dot(hidden[:, lines], upstream[...], TN)
        speed = (0.5 * MOMENTUM) * pair_w[1, lines].astype(F32) + weight_grad
        velocity[lines] = speed
        slow_w[lines] = 0.5 * slow_w[lines] - OUTER_RATE * (weight_grad + MOMENTUM * speed)
        for index, (kept, target) in enumerate(((slow_w, slow_out), (velocity, velocity_out))):
            copy = pltpu.make_async_copy(
                kept.at[lines], target.at[lines], store_sem.at[index, block]
            )
            copy.start()
            stores.append(copy)

    @pl.when(section != 0)
    def _():
        pltpu.make_async_copy(tokens_ref, tokens_ref, token_send).wait()
        gather_done(0)
        spread_done(grad, 1)

    @pl.when((section < sections - 1) & (section != 1))
    def _():
        spread_done(out, 0)

    @pl.when(section < sections - 1)
    def _():
        gather_done(1)

    for part in range(2):
        pltpu.make_async_copy(mate[part], mate[part], mate_recv.at[part]).wait()
    gossip_done()
    for copy in stores:
        copy.wait()


def local(sections, replicas, tokens, gate_weight, up_weight, slow_down, prev_outer, route, partner):
    rows = tokens.shape[1] * sections
    features = tokens.shape[2]
    units = gate_weight.shape[3]
    order = jnp.arange(replicas, dtype=jnp.int32)
    targets = route[:, 0]
    origins = jnp.sum(
        jnp.where(targets[:, :, None] == order, order[:, None], 0), axis=1, dtype=jnp.int32
    )
    across = min(16, replicas)
    down = replicas // across
    piece = (rows // down, features // across)
    share = (units // down, features // across)
    stride = 37 if replicas == 64 else 1
    torus = (4, 8, 2) if replicas == 64 else (1, replicas, 1)
    anywhere = pl.BlockSpec(memory_space=pl.ANY)
    dma = pltpu.SemaphoreType.DMA
    slow, velocity, mate_slow, mate_prev = pl.pallas_call(
        functools.partial(kernel, sections, replicas, stride, torus),
        out_shape=(
            jax.ShapeDtypeStruct((units, features), F32),
            jax.ShapeDtypeStruct((units, features), F32),
            jax.ShapeDtypeStruct((units, features), BF16),
            jax.ShapeDtypeStruct((units, features), BF16),
        ),
        in_specs=[pl.BlockSpec(memory_space=pltpu.SMEM)] * 3 + [pl.BlockSpec(memory_space=pltpu.HBM)] * 5,
        out_specs=(anywhere,) * 4,
        scratch_shapes=[
            pltpu.VMEM((features, units), BF16),
            pltpu.VMEM((features, units), BF16),
            pltpu.VMEM((units, features), F32),
            pltpu.VMEM((2, units, features), BF16),
            pltpu.VMEM((rows, features), BF16),
            pltpu.VMEM((rows, features), BF16),
            pltpu.VMEM((rows, features), BF16),
            pltpu.VMEM((rows, features), BF16),
            pltpu.VMEM((replicas, *piece), BF16),
            pltpu.VMEM((replicas, *piece), BF16),
            pltpu.VMEM((replicas, *piece), BF16),
            pltpu.VMEM((replicas, *piece), BF16),
            pltpu.VMEM((replicas, *share), BF16),
            pltpu.VMEM((replicas, *share), BF16),
            pltpu.VMEM((replicas, *share), BF16),
            pltpu.VMEM((replicas, *share), BF16),
            pltpu.VMEM((replicas, *share), BF16),
            pltpu.VMEM((replicas, *share), BF16),
            pltpu.VMEM((replicas, *share), BF16),
            pltpu.VMEM((replicas, *share), BF16),
            pltpu.VMEM((units, features), F32),
            pltpu.VMEM((rows, 1), F32),
            pltpu.VMEM((rows, units), F32),
            pltpu.VMEM((rows, units), F32),
            pltpu.VMEM((rows, units), BF16),
            dma((4,)),
            dma((2, units // 128)),
            dma,
            dma,
            dma((2,)),
            dma((2,)),
            dma((2,)),
            dma((2,)),
            dma((2,)),
            dma((4,)),
            dma((4,)),
            dma((2,)),
            pltpu.SemaphoreType.REGULAR,
        ],
        compiler_params=pltpu.CompilerParams(
            collective_id=0, has_side_effects=True, vmem_limit_bytes=40 * 2**20
        ),
        name="relay",
    )(
        origins,
        targets,
        partner,
        pltpu.with_memory_space_constraint(tokens[0], pltpu.HBM),
        pltpu.with_memory_space_constraint(gate_weight[0, 0], pltpu.HBM),
        pltpu.with_memory_space_constraint(up_weight[0, 0], pltpu.HBM),
        pltpu.with_memory_space_constraint(slow_down[0, 0], pltpu.HBM),
        pltpu.with_memory_space_constraint(prev_outer[0, 0], pltpu.HBM),
    )
    theirs = (0.5 * MOMENTUM) * mate_prev.astype(F32)
    new_slow = slow + (0.5 * mate_slow.astype(F32) - (OUTER_RATE * MOMENTUM) * theirs)
    new_outer = (velocity + theirs).astype(BF16)
    return (new_slow[None, None], new_outer[None, None])


def solution(mesh):
    sections, replicas = mesh.shape["section"], mesh.shape["replica"]
    own = P("section", "replica", None, None)
    return jax.shard_map(
        functools.partial(local, sections, replicas),
        mesh=mesh,
        in_specs=(P("replica", "section", None), own, own, own, own, P(), P()),
        out_specs=(own, own),
        check_vma=False,
    )
```
